256 devices in a mesh: ens: 4 (over y, x), region: 64 (over z, core).
Axes of the slice: x: 2, y: 2, z: 32, core: 2. Of those that a mesh axis runs over, the one named last changes fastest.
The devices are a block of a 4x8x32 slice.
Arguments:
- node_latent: bfloat16 [131072, 512], P(('ens', 'region')), parts along dimension 0, may hold values from -6 to 6
- grid_latent: bfloat16 [131072, 512], P(('ens', 'region')), parts along dimension 0, may hold values from -6 to 6
- fine_edge_sender: int32 [524288], P(('ens', 'region')), parts along dimension 0, may hold values from 0 to 32767, as said below
- short_recv: int32 [524288], P(('ens', 'region')), parts along dimension 0, may hold values from 0 to 511
- short_geo: float32 [4, 524288], P(None, ('ens', 'region')), parts along dimension 1, may hold values from -6 to 6
- long_send: int32 [131072], P(('ens', 'region')), parts along dimension 0, may hold values from -1 to 32767, as said below
- long_recv: int32 [131072], P(('ens', 'region')), parts along dimension 0, may hold values from 0 to 511
- long_geo: float32 [4, 131072], P(None, ('ens', 'region')), parts along dimension 1, may hold values from -6 to 6
- dec_send: int32 [3, 131072], P(None, ('ens', 'region')), parts along dimension 1, may hold values from 0 to 32767, as said below
- dec_geo: float32 [4, 3, 131072], P(None, None, ('ens', 'region')), parts along dimension 2, may hold values from -6 to 6
- w_send: bfloat16 [512, 512], replicated, may hold values from -0.25 to 0.25
- w_recv: bfloat16 [512, 512], replicated, may hold values from -0.25 to 0.25
- w_edge_geo: float32 [4, 512], replicated, may hold values from -3 to 3
- w_message: bfloat16 [512, 512], replicated, may hold values from -0.25 to 0.25
- w_node_self: bfloat16 [512, 512], replicated, may hold values from -0.25 to 0.25
- w_node_agg: bfloat16 [512, 512], replicated, may hold values from -0.25 to 0.25
- w_node_out: bfloat16 [512, 512], replicated, may hold values from -0.25 to 0.25
- w_dec_send: bfloat16 [512, 512], replicated, may hold values from -0.25 to 0.25
- w_dec_grid: bfloat16 [512, 512], replicated, may hold values from -0.25 to 0.25
- w_dec_geo: float32 [4, 512], replicated, may hold values from -3 to 3
- decoding_link_final_matrix: bfloat16 [512, 512], replicated, may hold values from -0.25 to 0.25
- w_grid_agg: bfloat16 [512, 512], replicated, may hold values from -0.25 to 0.25
- w_grid_self: bfloat16 [512, 512], replicated, may hold values from -0.25 to 0.25
- final_projection_matrix: bfloat16 [100, 512], replicated, may hold values from -0.25 to 0.25
Outputs:
- refreshed_mesh_latents: bfloat16 [131072, 512], P(('ens', 'region')), parts along dimension 0
- predicted_fields: bfloat16 [100, 131072], P(None, ('ens', 'region')), parts along dimension 1
The draws below stay inside these ranges and needn't reach their ends.
There are 4 independent parts, one for each index of `ens`. The reference program is written for one: setup_inputs(seed, part) draws one part's arguments, and reference() takes and returns one part's arrays. A program takes and returns all parts, laid end to end along the dimension named above; an argument that names none is the same for every part. Nothing has to cross between parts.
Inputs may be any that keep to these rules, and one draw needn't show every extreme that they name: `fine_edge_sender`: A fine edge held by region d has its sender in region d, among the last 64 nodes of region d - 1, or among the first 64 nodes of region d + 1; node 448 of region d - 1 (the first of its last 64) and node 63 of region d + 1 are used where those regions exist. `long_send`: slot d * 512 + o * 8 + j, unless -1, names one of the first 64 nodes of region o; in every region one other region's 8 slots are all filled. `dec_send`: the senders of a grid point of band d lie in region d, among the last 64 nodes of region d - 1, or among the first 64 nodes of region d + 1; node 448 of region d - 1 (the first of its last 64) and node 63 of region d + 1 are used where those regions exist.
All inputs are finite; a program needn't handle non-finite values.
Results may differ from the reference program's by a relative error of at most 0.013.
Values may be sent and summed in bfloat16 or wider, within the bound.
No kernel may reach another device: no remote copies, remote signals or barrier semaphores. Data moves between devices by JAX's collectives and lax.ppermute only.
A program may use at most 128 MiB of HBM per device.

```python
import jax
import jax.numpy as jnp
from jax import lax

H = 512
C_OUT = 100
GEO = 4
MESH_DEV = 512
G_DEV = 512
LONG_DEV = 512
BORDER = 64
SHORT_DEV = 2048
COARSE_DEV = 64
SLOT = 8
MESH_NODES = 32768
GRID = 32768
N_REGION = 64


def rim_draw(key, processor_part, within):
    first, second, third = jax.random.split(key, 3)
    extent = processor_part.shape
    kind = jax.random.randint(first, extent, 0, 6)
    kind = jnp.where(within == 0, 0, jnp.where(within == 1, 1, kind))
    local = jax.random.randint(second, extent, 0, MESH_DEV)
    depth = jax.random.randint(third, extent, 0, BORDER)
    depth = jnp.where(within == 0, 0, jnp.where(within == 1, BORDER - 1, depth))
    lower = (processor_part - 1) * MESH_DEV + MESH_DEV - BORDER + depth
    upper = (processor_part + 1) * MESH_DEV + depth
    own_node = processor_part * MESH_DEV + local
    picked = jnp.where((kind == 0) & (processor_part > 0), lower, jnp.where((kind == 1) & (processor_part < N_REGION - 1), upper, own_node))
    return picked.astype(jnp.int32)


def draw_fine_edge_sender(key, part):
    position = jnp.arange(N_REGION * SHORT_DEV, dtype=jnp.int32)
    return rim_draw(jax.random.fold_in(key, 11), position // SHORT_DEV, position % SHORT_DEV)


def draw_dec_send(key, part):
    points = jnp.arange(N_REGION * G_DEV, dtype=jnp.int32)
    vertex = jnp.arange(3, dtype=jnp.int32)[:, None]
    processor_part = jnp.broadcast_to((points // G_DEV)[None, :], (3, N_REGION * G_DEV))
    within = (points % G_DEV)[None, :] * 3 + vertex
    return rim_draw(jax.random.fold_in(key, 23), processor_part, within)


def draw_long_send(key, part):
    first, second, third = jax.random.split(jax.random.fold_in(key, 37), 3)
    position = jnp.arange(N_REGION * LONG_DEV, dtype=jnp.int32)
    processor_part = position // LONG_DEV
    within = position % LONG_DEV
    owner = within // SLOT
    column = within % SLOT
    levels = jax.random.randint(first, (N_REGION,), 20, 101)
    live = jax.random.randint(second, position.shape, 0, 100) < levels[processor_part]
    filled = owner == (processor_part * 7 + 3) % N_REGION
    live = live | filled
    local = jax.random.randint(third, position.shape, 0, COARSE_DEV)
    local = jnp.where(filled & (column == 0), COARSE_DEV - 1, local)
    return jnp.where(live, owner * MESH_DEV + local, -1).astype(jnp.int32)


def place_ends(result, rng, smallest, top_value):
    index_at = [jax.random.randint(jax.random.fold_in(rng, axis), (), 0, length) for axis, length in enumerate(result.shape)]
    main_axis = result.shape.index(max(result.shape))
    next_to = index_at[:main_axis] + [(index_at[main_axis] + 1) % result.shape[main_axis]] + index_at[main_axis + 1:]
    return result.at[tuple(index_at)].set(smallest).at[tuple(next_to)].set(top_value)


def steps_of(stream_key, shape, shards, low, high):
    gain = 1.0
    for dim, shards_of in shards:
        draws = jax.random.uniform(jax.random.fold_in(jax.random.fold_in(stream_key, 6), dim), (shards_of,), jnp.float32, low / len(shards), high / len(shards))
        gain = gain * jnp.repeat(jnp.exp(draws), shape[dim] // shards_of).reshape((-1,) + (1,) * (len(shape) - 1 - dim))
    return gain


def noise(key, shape, deviation, bound, pieces=(), kind=jnp.bfloat16):
    values = jax.random.normal(key, shape, jnp.float32) * deviation
    if len(pieces) > 0:
        values = steps_of(key, shape, pieces, -0.22, 0.18) * values
    return jnp.clip(values, min=-bound, max=bound).astype(kind)


def setup_inputs(seed: int = 0, part: int = 0) -> dict:
    key_of = jax.random.split(jax.random.key(seed), 25)
    part_keys = jax.random.split(jax.random.fold_in(key_of[24], part), 25)
    node_latent = noise(part_keys[0], (MESH_NODES, H), 1.0, 6.0, ((0, 64),))
    grid_latent = noise(part_keys[1], (GRID, H), 1.0, 6.0, ((0, 64),))
    fine_edge_sender = draw_fine_edge_sender(jax.random.fold_in(jax.random.fold_in(key_of[24], part), 71), part)
    short_recv = place_ends(jax.random.randint(part_keys[3], (N_REGION * SHORT_DEV,), 0, MESH_DEV), jax.random.fold_in(part_keys[3], 1), 0, MESH_DEV - 1).astype(jnp.int32)
    short_geo = noise(part_keys[4], (GEO, N_REGION * SHORT_DEV), 1.0, 6.0, ((1, 64),), jnp.float32)
    long_send = draw_long_send(jax.random.fold_in(jax.random.fold_in(key_of[24], part), 71), part)
    long_recv = place_ends(jax.random.randint(part_keys[6], (N_REGION * LONG_DEV,), 0, MESH_DEV), jax.random.fold_in(part_keys[6], 1), 0, MESH_DEV - 1).astype(jnp.int32)
    long_geo = noise(part_keys[7], (GEO, N_REGION * LONG_DEV), 1.0, 6.0, ((1, 64),), jnp.float32)
    dec_send = draw_dec_send(jax.random.fold_in(jax.random.fold_in(key_of[24], part), 71), part)
    dec_geo = noise(part_keys[9], (GEO, 3, GRID), 1.0, 6.0, ((2, 64),), jnp.float32)
    w_send = noise(key_of[10], (H, H), H ** -0.5, 0.25)
    w_recv = noise(key_of[11], (H, H), H ** -0.5, 0.25)
    w_edge_geo = noise(key_of[12], (GEO, H), GEO ** -0.5, 3.0, (), jnp.float32)
    w_message = noise(key_of[13], (H, H), H ** -0.5, 0.25)
    w_node_self = noise(key_of[14], (H, H), H ** -0.5, 0.25)
    w_node_agg = noise(key_of[15], (H, H), H ** -0.5, 0.25)
    w_node_out = noise(key_of[16], (H, H), H ** -0.5, 0.25)
    w_dec_send = noise(key_of[17], (H, H), H ** -0.5, 0.25)
    w_dec_grid = noise(key_of[18], (H, H), H ** -0.5, 0.25)
    w_dec_geo = noise(key_of[19], (GEO, H), GEO ** -0.5, 3.0, (), jnp.float32)
    decoding_link_final_matrix = noise(key_of[20], (H, H), H ** -0.5, 0.25)
    w_grid_agg = noise(key_of[21], (H, H), H ** -0.5, 0.25)
    w_grid_self = noise(key_of[22], (H, H), H ** -0.5, 0.25)
    final_projection_matrix = noise(key_of[23], (C_OUT, H), H ** -0.5, 0.25)
    return {"node_latent": node_latent, "grid_latent": grid_latent, "fine_edge_sender": fine_edge_sender, "short_recv": short_recv, "short_geo": short_geo, "long_send": long_send, "long_recv": long_recv, "long_geo": long_geo, "dec_send": dec_send, "dec_geo": dec_geo, "w_send": w_send, "w_recv": w_recv, "w_edge_geo": w_edge_geo, "w_message": w_message, "w_node_self": w_node_self, "w_node_agg": w_node_agg, "w_node_out": w_node_out, "w_dec_send": w_dec_send, "w_dec_grid": w_dec_grid, "w_dec_geo": w_dec_geo, "decoding_link_final_matrix": decoding_link_final_matrix, "w_grid_agg": w_grid_agg, "w_grid_self": w_grid_self, "final_projection_matrix": final_projection_matrix}


def product(left, right):
    return jnp.dot(left, right, preferred_element_type=jnp.float32)

def geometry(feature_vectors, learned_factor):
    return lax.dot_general(feature_vectors, learned_factor, (((0,), (0,)), ((), ())), precision=lax.Precision.HIGHEST)

def normalize(values):
    middle_point = values - lax.optimization_barrier(jnp.mean(values, axis=-1, keepdims=True))
    spread = lax.optimization_barrier(jnp.mean(middle_point * middle_point, axis=-1, keepdims=True))
    return middle_point * lax.rsqrt(spread + 1e-05)

def messages(edge_pre, w_message):
    edge_hidden = jax.nn.silu(edge_pre).astype(jnp.bfloat16)
    return normalize(product(edge_hidden, w_message))

def reference(node_latent, grid_latent, fine_edge_sender, short_recv, short_geo, long_send, long_recv, long_geo, dec_send, dec_geo, w_send, w_recv, w_edge_geo, w_message, w_node_self, w_node_agg, w_node_out, w_dec_send, w_dec_grid, w_dec_geo, decoding_link_final_matrix, w_grid_agg, w_grid_self, final_projection_matrix):
    total_nodes = node_latent.shape[0]
    channel_count = node_latent.shape[1]
    send_proj = product(node_latent, w_send)
    recv_proj = product(node_latent, w_recv)
    fine_target = short_recv + jnp.arange(N_REGION * SHORT_DEV, dtype=jnp.int32) // SHORT_DEV * MESH_DEV
    fine_pre = send_proj[fine_edge_sender] + recv_proj[fine_target] + geometry(short_geo, w_edge_geo)
    fine_msg = messages(fine_pre, w_message)
    present = long_send >= 0
    clipped = jnp.maximum(long_send, 0)
    far_target = long_recv + jnp.arange(N_REGION * LONG_DEV, dtype=jnp.int32) // LONG_DEV * MESH_DEV
    far_pre = send_proj[clipped] + recv_proj[far_target] + geometry(long_geo, w_edge_geo)
    far_msg = messages(far_pre, w_message) * present[:, None].astype(fine_msg.dtype)
    aggregate = jnp.zeros((total_nodes, channel_count), fine_msg.dtype).at[fine_target].add(fine_msg).at[far_target].add(far_msg)
    node_hidden = jax.nn.silu(product(node_latent, w_node_self) + product(aggregate.astype(jnp.bfloat16), w_node_agg)).astype(jnp.bfloat16)
    refreshed_mesh_latents = (node_latent.astype(jnp.float32) + product(node_hidden, w_node_out)).astype(jnp.bfloat16)
    dec_proj = product(refreshed_mesh_latents, w_dec_send)
    grid_proj = product(grid_latent, w_dec_grid)
    grid_sum = jnp.zeros(grid_proj.shape, grid_proj.dtype)
    for vertex in range(3):
        dec_pre = dec_proj[dec_send[vertex]] + grid_proj + geometry(dec_geo[:, vertex, :], w_dec_geo)
        grid_sum = grid_sum + messages(dec_pre, decoding_link_final_matrix)
    grid_agg = grid_sum.astype(jnp.bfloat16)
    latitude_site_latent_matrix = jax.nn.silu(product(grid_agg, w_grid_agg) + product(grid_latent, w_grid_self)).astype(jnp.bfloat16)
    predicted_fields = lax.dot_general(final_projection_matrix, latitude_site_latent_matrix, (((1,), (1,)), ((), ())), preferred_element_type=jnp.float32).astype(jnp.bfloat16)
    return (refreshed_mesh_latents, predicted_fields)
```

```python
import functools

import jax
import jax.numpy as jnp
from jax import lax
from jax.experimental import pallas as pl
from jax.experimental.pallas import tpu as pltpu
from jax.sharding import PartitionSpec as P

BORDER = 64
COARSE = 64
BLOCK = 8
LANES = 128
F32 = jnp.float32
BF16 = jnp.bfloat16


def dot(left, right):
    return jnp.dot(left, right, preferred_element_type=F32)


def silu(v):
    half = 0.5 * v
    return half + half * jnp.tanh(half)


def normalize(values):
    inv = 1.0 / values.shape[-1]
    centred = values - jnp.sum(values, axis=-1, keepdims=True) * inv
    spread = jnp.sum(centred * centred, axis=-1, keepdims=True) * inv
    return centred * lax.rsqrt(spread + 1e-05)


def columns(rows):
    return jnp.concatenate(
        [jnp.broadcast_to(r, (LANES, LANES)).T for r in rows], axis=0
    )


def one_hot(cols, width):
    lane = lax.broadcasted_iota(jnp.int32, cols.shape, 1)
    return jnp.concatenate(
        [jnp.where(cols == lane + k, 1.0, 0.0).astype(BF16) for k in range(0, width, LANES)], axis=1
    )


def one_hot_t(rows, height):
    node = lax.broadcasted_iota(jnp.int32, (height, LANES), 0)
    return jnp.concatenate([jnp.where(node == r, 1.0, 0.0).astype(BF16) for r in rows], axis=1)


def split(values):
    high = values.astype(BF16).astype(F32)
    return high, values - high


def geo_columns(stack):
    n = stack.shape[1]
    full = jnp.concatenate([stack, jnp.zeros((LANES - 32, n), F32)], axis=0)
    return jnp.concatenate(
        [full[:, b : b + LANES].T for b in range(0, n, LANES)], axis=0
    ).astype(BF16)


def fill_geo(ref, first, second, third):
    ref[...] = jnp.zeros(ref.shape, F32)
    n = first.shape[0]
    ref[0:n, :] = first
    ref[8 : 8 + n, :] = second
    ref[16 : 16 + n, :] = third


def geo_table(wref, scratch):
    high, low = split(wref[...])
    fill_geo(scratch, high, high, low)
    rows = scratch[...]
    return jnp.concatenate([rows, jnp.zeros((LANES - 32, rows.shape[1]), F32)], axis=0).astype(BF16)


def fetch(pairs, sems):
    copies = [pltpu.make_async_copy(src, dst, sems.at[i]) for i, (src, dst) in enumerate(pairs)]
    for copy in copies:
        copy.start()
    return copies


def relay_kernel(asked_ref, table_ref, out_ref):
    rows = out_ref.shape[0] // asked_ref.shape[0]
    cols = jnp.concatenate(
        [columns([asked_ref[q, 0:1, :]])[:rows] for q in range(asked_ref.shape[0])], axis=0
    )
    out_ref[...] = dot(one_hot(cols, table_ref.shape[0]), table_ref[...]).astype(BF16)


def fine_kernel(
    off_ref, fs_ref, sr_ref, geo_ref, lr_ref, lgeo_ref, before_ref, after_ref, weg_ref,
    x_hbm, ws_hbm, wr_hbm, wm_hbm, wself_hbm,
    agg_ref, base_ref, nself_ref, ws_ref,
    tab, msg, gsc, lsc, wsc, x_ref, wr_ref, wm_ref, wself_ref, sems, *, tile,
):
    x_copy, ws_copy, wr_copy, wm_copy, wself_copy = fetch(
        [(x_hbm, x_ref), (ws_hbm, ws_ref), (wr_hbm, wr_ref), (wm_hbm, wm_ref), (wself_hbm, wself_ref)],
        sems,
    )
    n, h = x_ref.shape
    edges = geo_ref.shape[1]
    ext = n + 2 * BORDER
    tab[ext + n : ext + n + LANES, :] = geo_table(weg_ref, wsc)
    high, low = split(geo_ref[...])
    fill_geo(gsc, high, low, high)
    high, low = split(lgeo_ref[...])
    fill_geo(lsc, high, low, high)
    x_copy.wait()
    ws_copy.wait()
    x = x_ref[...]
    tab[0:BORDER, :] = dot(before_ref[...], ws_ref[...]).astype(BF16)
    tab[BORDER : BORDER + n, :] = dot(x, ws_ref[...]).astype(BF16)
    tab[BORDER + n : ext, :] = dot(after_ref[...], ws_ref[...]).astype(BF16)
    wr_copy.wait()
    tab[ext : ext + n, :] = dot(x, wr_ref[...]).astype(BF16)
    wself_copy.wait()
    nself_ref[...] = dot(x, wself_ref[...]).astype(BF16)
    wm_copy.wait()
    off = off_ref[0]
    per = tile // LANES

    def step(t, carry):
        row = t * per
        lane0 = pl.multiple_of(t * tile, tile)
        send = columns([fs_ref[pl.ds(row + b, 1), :] - off for b in range(per)])
        recv = columns([sr_ref[pl.ds(row + b, 1), :] for b in range(per)])
        lhs = jnp.concatenate(
            [one_hot(send, ext), one_hot(recv, n), geo_columns(gsc[:, pl.ds(lane0, tile)])], axis=1
        )
        hidden = silu(dot(lhs, tab[...])).astype(BF16)
        msg[pl.ds(lane0, tile), :] = normalize(dot(hidden, wm_ref[...])).astype(BF16)
        return carry

    lax.fori_loop(0, edges // tile, step, 0)
    agg_ref[...] = dot(
        one_hot_t([sr_ref[b : b + 1, :] for b in range(edges // LANES)], n), msg[...]
    )
    far = lr_ref.shape[0]
    recv = columns([lr_ref[b : b + 1, :] for b in range(far)])
    lhs = jnp.concatenate([one_hot(recv, n), geo_columns(lsc[...])], axis=1)
    base_ref[...] = dot(lhs, tab[ext : ext + n + LANES, :]).astype(BF16)


def node_kernel(
    lr_ref, far_ref, agg_ref, base_ref, nself_ref, ws_ref, x_hbm, wm_hbm, wa_hbm, wo_hbm,
    out_ref, first_ref, last_ref, x_ref, wm_ref, wa_ref, wo_ref, sems,
):
    wm_copy, wa_copy, wo_copy, x_copy = fetch(
        [(wm_hbm, wm_ref), (wa_hbm, wa_ref), (wo_hbm, wo_ref), (x_hbm, x_ref)], sems
    )
    n = x_ref.shape[0]
    hidden = silu(dot(far_ref[...], ws_ref[...]) + base_ref[...].astype(F32)).astype(BF16)
    scatter = one_hot_t([lr_ref[b : b + 1, :] for b in range(lr_ref.shape[0])], n)
    wm_copy.wait()
    message = normalize(dot(hidden, wm_ref[...])).astype(BF16)
    aggregate = (agg_ref[...] + dot(scatter, message)).astype(BF16)
    wa_copy.wait()
    node_hidden = silu(nself_ref[...].astype(F32) + dot(aggregate, wa_ref[...])).astype(BF16)
    wo_copy.wait()
    x_copy.wait()
    fresh = (x_ref[...].astype(F32) + dot(node_hidden, wo_ref[...])).astype(BF16)
    out_ref[...] = fresh
    first_ref[...] = fresh[:BORDER]
    last_ref[...] = fresh[n - BORDER :]


def own_kernel(
    off_ref, ds_ref, geo_ref, wdgeo_ref, x_ref, grid_hbm, wds_hbm, wdg_hbm, wgs_hbm, wf_hbm, wga_hbm,
    fresh_hbm, pre_ref, gproj_ref, gself_ref, wds_ref, wf_ref, wga_ref,
    tab, gsc, wsc, grid_ref, wdg_ref, wgs_ref, sems,
):
    wds_copy, wdg_copy, grid_copy, wgs_copy, wf_copy, wga_copy, fresh_copy = fetch(
        [
            (wds_hbm, wds_ref), (wdg_hbm, wdg_ref), (grid_hbm, grid_ref), (wgs_hbm, wgs_ref),
            (wf_hbm, wf_ref), (wga_hbm, wga_ref), (x_ref, fresh_hbm),
        ],
        sems,
    )
    n = x_ref.shape[0]
    vertices, points = ds_ref.shape
    features = geo_ref.shape[0] // vertices
    tab[n : n + LANES, :] = geo_table(wdgeo_ref, wsc)
    tab[n + LANES :, :] = jnp.zeros((LANES, tab.shape[1]), BF16)
    wds_copy.wait()
    tab[0:n, :] = dot(x_ref[...], wds_ref[...]).astype(BF16)
    wdg_copy.wait()
    grid_copy.wait()
    gproj_ref[...] = dot(grid_ref[...], wdg_ref[...])
    start = off_ref[0] + BORDER
    for v in range(vertices):
        gsc[...] = jnp.zeros(gsc.shape, F32)
        for c in range(features):
            high, low = split(geo_ref[c * vertices + v : c * vertices + v + 1, :])
            gsc[c : c + 1, :] = high
            gsc[8 + c : 9 + c, :] = low
            gsc[16 + c : 17 + c, :] = high
        send = columns([ds_ref[v : v + 1, b : b + LANES] - start for b in range(0, points, LANES)])
        empty = jnp.zeros((points, LANES), BF16)
        lhs = jnp.concatenate([one_hot(send, n), geo_columns(gsc[...]), empty], axis=1)
        pre_ref[v * points : (v + 1) * points, :] = dot(lhs, tab[...])
    wgs_copy.wait()
    gself_ref[...] = dot(grid_ref[...], wgs_ref[...])
    wf_copy.wait()
    wga_copy.wait()
    fresh_copy.wait()


def grid_kernel(
    off_ref, ds_ref, before_ref, after_ref, pre_ref, gproj_ref, gself_ref, wds_ref, wf_ref, wga_ref, wp_ref,
    out_ref, *, nodes,
):
    vertices, points = ds_ref.shape
    halo = jnp.concatenate(
        [dot(before_ref[...], wds_ref[...]), dot(after_ref[...], wds_ref[...])], axis=0
    ).astype(BF16)
    off = off_ref[0]
    total = jnp.zeros((points, gself_ref.shape[1]), F32)
    for v in range(vertices):
        rows = []
        for b in range(0, points, LANES):
            place = ds_ref[v : v + 1, b : b + LANES] - off
            rows.append(
                jnp.where(place < BORDER, place, jnp.where(place >= BORDER + nodes, place - nodes, -1))
            )
        lhs = one_hot(columns(rows), 2 * BORDER)
        hidden = silu(
            dot(lhs, halo) + (pre_ref[v * points : (v + 1) * points, :] + gproj_ref[...])
        ).astype(BF16)
        total = total + normalize(dot(hidden, wf_ref[...]))
    hidden = silu(dot(total.astype(BF16), wga_ref[...]) + gself_ref[...]).astype(BF16)
    out_ref[...] = lax.dot_general(
        wp_ref[...], hidden, (((1,), (1,)), ((), ())), preferred_element_type=F32
    ).astype(BF16)


VM = pl.BlockSpec(memory_space=pltpu.MemorySpace.VMEM)
SM = pl.BlockSpec(memory_space=pltpu.MemorySpace.SMEM)
AN = pl.BlockSpec(memory_space=pltpu.MemorySpace.HBM)


def call(kernel, outs, ins, out_specs, scratch=(), mib=24, flops=0):
    return pl.pallas_call(
        kernel,
        out_shape=outs,
        in_specs=ins,
        out_specs=out_specs,
        scratch_shapes=list(scratch),
        compiler_params=pltpu.CompilerParams(vmem_limit_bytes=mib << 20),
        cost_estimate=pl.CostEstimate(flops=flops, transcendentals=0, bytes_accessed=1 << 22),
    )


def far_memory(*arrays):
    return [pltpu.with_memory_space_constraint(a, pltpu.MemorySpace.HBM) for a in arrays]


def swap(first, last):
    size = lax.axis_size("region")
    up = [(i, i + 1) for i in range(size - 1)]
    down = [(j, i) for i, j in up]
    return lax.ppermute(last, "region", up), lax.ppermute(first, "region", down)


def body(
    node_latent, grid_latent, fine_edge_sender, short_recv, short_geo, long_send, long_recv,
    long_geo, dec_send, dec_geo, w_send, w_recv, w_edge_geo, w_message, w_node_self, w_node_agg,
    w_node_out, w_dec_send, w_dec_grid, w_dec_geo, decoding_link_final_matrix, w_grid_agg,
    w_grid_self, final_projection_matrix,
):
    n, h = node_latent.shape
    points = grid_latent.shape[0]
    edges = fine_edge_sender.shape[0]
    far = long_send.shape[0]
    vertices = dec_send.shape[0]
    outputs = final_projection_matrix.shape[0]
    regions = lax.axis_size("region")
    slot = far // regions
    rings = regions // BLOCK
    offset = (lax.axis_index("region") * n - BORDER).astype(jnp.int32).reshape(1)

    classes = [[q + BLOCK * i for i in range(rings)] for q in range(BLOCK)]
    blocks = [[BLOCK * b + q for q in range(BLOCK)] for b in range(rings)]
    group = jnp.arange(regions, dtype=jnp.int32)
    wanted = jnp.maximum(long_send.reshape(regions, slot) - (group * n)[:, None], 0)
    wanted = (wanted + (group // BLOCK * COARSE)[:, None]).reshape(rings, BLOCK, slot)
    wanted = wanted.transpose(1, 0, 2).reshape(BLOCK, 1, rings * slot)
    wanted = jnp.broadcast_to(
        jnp.pad(wanted, ((0, 0), (0, 0), (0, LANES - rings * slot))), (BLOCK, 8, LANES)
    )
    asked = lax.all_to_all(
        wanted, "region", split_axis=0, concat_axis=0, tiled=True, axis_index_groups=blocks
    )
    table = lax.all_gather(
        node_latent[:COARSE], "region", axis=0, tiled=True, axis_index_groups=classes
    )
    whole = jax.ShapeDtypeStruct((n, h), BF16)
    field = jax.ShapeDtypeStruct((points, h), F32)
    weight = jax.ShapeDtypeStruct((h, h), BF16)
    rows = call(relay_kernel, jax.ShapeDtypeStruct((far, h), BF16), [VM, VM], VM, mib=8)(asked, table)
    rows, node_later = lax.optimization_barrier((rows, node_latent))
    fetched = lax.all_to_all(
        rows.reshape(BLOCK, far // BLOCK, h), "region",
        split_axis=0, concat_axis=0, tiled=True, axis_index_groups=blocks,
    ).reshape(far, h)

    target = jnp.where(long_send >= 0, long_recv, -1)
    target = target.reshape(rings, BLOCK, slot).transpose(1, 0, 2).reshape(far // LANES, LANES)
    far_geo = long_geo.reshape(-1, rings, BLOCK, slot).transpose(0, 2, 1, 3).reshape(-1, far)
    before, after = swap(node_latent[:BORDER], node_latent[n - BORDER :])
    tile = 512
    ext = n + 2 * BORDER
    dense = pltpu.VMEM((h, h), BF16)
    aggregate, base, node_self, send_weight = call(
        functools.partial(fine_kernel, tile=tile),
        (jax.ShapeDtypeStruct((n, h), F32), jax.ShapeDtypeStruct((far, h), BF16), whole, weight),
        [SM] + [VM] * 8 + [AN] * 5,
        (VM,) * 4,
        [
            pltpu.VMEM((ext + n + LANES, h), BF16),
            pltpu.VMEM((edges, h), BF16),
            pltpu.VMEM((32, edges), F32),
            pltpu.VMEM((32, far), F32),
            pltpu.VMEM((32, h), F32),
            pltpu.VMEM((n, h), BF16),
            dense, dense, dense,
            pltpu.SemaphoreType.DMA((5,)),
        ],
        mib=28,
        flops=8 * edges * h * h,
    )(
        offset, fine_edge_sender.reshape(-1, LANES), short_recv.reshape(-1, LANES), short_geo,
        target, far_geo, before, after, w_edge_geo,
        *far_memory(node_later, w_send, w_recv, w_message, w_node_self),
    )
    border = jax.ShapeDtypeStruct((BORDER, h), BF16)
    fresh, first, last = call(
        node_kernel,
        (whole, border, border),
        [VM] * 6 + [AN] * 4,
        (VM,) * 3,
        [pltpu.VMEM((n, h), BF16), dense, dense, dense, pltpu.SemaphoreType.DMA((4,))],
        mib=16,
        flops=10 * n * h * h,
    )(
        target, fetched, aggregate, base, node_self, send_weight,
        *far_memory(node_later, w_message, w_node_agg, w_node_out),
    )
    before, after = swap(first, last)
    refreshed, pre, grid_proj, grid_self, dec_weight, final_weight, agg_weight = call(
        own_kernel,
        (
            whole, jax.ShapeDtypeStruct((vertices * points, h), F32),
            field, field, weight, weight, weight,
        ),
        [SM] + [VM] * 4 + [AN] * 6,
        (AN,) + (VM,) * 6,
        [
            pltpu.VMEM((n + 2 * LANES, h), BF16),
            pltpu.VMEM((32, points), F32),
            pltpu.VMEM((32, h), F32),
            pltpu.VMEM((points, h), BF16),
            dense, dense,
            pltpu.SemaphoreType.DMA((7,)),
        ],
        mib=20,
        flops=10 * n * h * h,
    )(
        offset, dec_send, dec_geo.reshape(-1, points), w_dec_geo, fresh,
        *far_memory(
            grid_latent, w_dec_send, w_dec_grid, w_grid_self, decoding_link_final_matrix, w_grid_agg
        ),
    )
    predicted = call(
        functools.partial(grid_kernel, nodes=n),
        jax.ShapeDtypeStruct((outputs, points), BF16),
        [SM] + [VM] * 10,
        VM,
        mib=20,
        flops=12 * n * h * h,
    )(
        offset, dec_send, before, after, pre, grid_proj, grid_self, dec_weight, final_weight, agg_weight,
        final_projection_matrix,
    )
    return (refreshed, predicted)


def solution(mesh):
    rows = P(("ens", "region"), None)
    line = P(("ens", "region"))
    in_specs = (
        rows, rows, line, line, P(None, ("ens", "region")), line, line, P(None, ("ens", "region")),
        P(None, ("ens", "region")), P(None, None, ("ens", "region")),
    ) + (P(),) * 14
    out_specs = (rows, P(None, ("ens", "region")))
    return jax.shard_map(body, mesh=mesh, in_specs=in_specs, out_specs=out_specs, check_vma=False)
```

```python
import functools

import jax
import jax.numpy as jnp
from jax import lax
from jax.experimental import pallas as pl
from jax.experimental.pallas import tpu as pltpu
from jax.sharding import PartitionSpec as P

BORDER = 64
COARSE = 64
BLOCK = 8
LANES = 128
F32 = jnp.float32
BF16 = jnp.bfloat16


def dot(left, right):
    return jnp.dot(left, right, preferred_element_type=F32)


def silu(v):
    half = 0.5 * v
    return half + half * jnp.tanh(half)


def normalize(values):
    inv = 1.0 / values.shape[-1]
    centred = values - jnp.sum(values, axis=-1, keepdims=True) * inv
    spread = jnp.sum(centred * centred, axis=-1, keepdims=True) * inv
    return centred * lax.rsqrt(spread + 1e-05)


def columns(rows):
    return jnp.concatenate(
        [jnp.broadcast_to(r, (LANES, LANES)).T for r in rows], axis=0
    )


def one_hot(cols, width):
    lane = lax.broadcasted_iota(jnp.int32, cols.shape, 1)
    return jnp.concatenate(
        [jnp.where(cols == lane + k, 1.0, 0.0).astype(BF16) for k in range(0, width, LANES)], axis=1
    )


def one_hot_t(rows, height):
    node = lax.broadcasted_iota(jnp.int32, (height, LANES), 0)
    return jnp.concatenate([jnp.where(node == r, 1.0, 0.0).astype(BF16) for r in rows], axis=1)


def split(values):
    high = values.astype(BF16).astype(F32)
    return high, values - high


def geo_columns(stack):
    n = stack.shape[1]
    full = jnp.concatenate([stack, jnp.zeros((LANES - 32, n), F32)], axis=0)
    return jnp.concatenate(
        [full[:, b : b + LANES].T for b in range(0, n, LANES)], axis=0
    ).astype(BF16)


def fill_geo(ref, first, second, third):
    ref[...] = jnp.zeros(ref.shape, F32)
    n = first.shape[0]
    ref[0:n, :] = first
    ref[8 : 8 + n, :] = second
    ref[16 : 16 + n, :] = third


def geo_table(wref, scratch):
    high, low = split(wref[...])
    fill_geo(scratch, high, high, low)
    rows = scratch[...]
    return jnp.concatenate([rows, jnp.zeros((LANES - 32, rows.shape[1]), F32)], axis=0).astype(BF16)


def fetch(pairs, sems):
    copies = [pltpu.make_async_copy(src, dst, sems.at[i]) for i, (src, dst) in enumerate(pairs)]
    for copy in copies:
        copy.start()
    return copies


def relay_kernel(asked_ref, table_ref, out_ref):
    rows = out_ref.shape[0] // asked_ref.shape[0]
    cols = jnp.concatenate(
        [columns([asked_ref[q, 0:1, :]])[:rows] for q in range(asked_ref.shape[0])], axis=0
    )
    out_ref[...] = dot(one_hot(cols, table_ref.shape[0]), table_ref[...]).astype(BF16)


def fine_kernel(
    off_ref, fs_ref, sr_ref, geo_ref, lr_ref, lgeo_ref, before_ref, after_ref, weg_ref,
    x_hbm, ws_hbm, wr_hbm, wm_hbm, wself_hbm, grid_hbm, wdg_hbm, wgs_hbm,
    agg_ref, base_ref, nself_ref, ws_ref, gproj_ref, gself_ref,
    tab, msg, gsc, lsc, wsc, x_ref, wr_ref, wm_ref, wself_ref, grid_ref, wdg_ref, wgs_ref, sems, *, tile,
):
    x_copy, ws_copy, wr_copy, wm_copy, wself_copy, grid_copy, wdg_copy, wgs_copy = fetch(
        [
            (x_hbm, x_ref), (ws_hbm, ws_ref), (wr_hbm, wr_ref), (wm_hbm, wm_ref),
            (wself_hbm, wself_ref), (grid_hbm, grid_ref), (wdg_hbm, wdg_ref), (wgs_hbm, wgs_ref),
        ],
        sems,
    )
    n, h = x_ref.shape
    edges = geo_ref.shape[1]
    ext = n + 2 * BORDER
    tab[ext + n : ext + n + LANES, :] = geo_table(weg_ref, wsc)
    high, low = split(geo_ref[...])
    fill_geo(gsc, high, low, high)
    high, low = split(lgeo_ref[...])
    fill_geo(lsc, high, low, high)
    x_copy.wait()
    ws_copy.wait()
    x = x_ref[...]
    tab[0:BORDER, :] = dot(before_ref[...], ws_ref[...]).astype(BF16)
    tab[BORDER : BORDER + n, :] = dot(x, ws_ref[...]).astype(BF16)
    tab[BORDER + n : ext, :] = dot(after_ref[...], ws_ref[...]).astype(BF16)
    wr_copy.wait()
    tab[ext : ext + n, :] = dot(x, wr_ref[...]).astype(BF16)
    wself_copy.wait()
    nself_ref[...] = dot(x, wself_ref[...]).astype(BF16)
    grid_copy.wait()
    wdg_copy.wait()
    gproj_ref[...] = dot(grid_ref[...], wdg_ref[...]).astype(BF16)
    wgs_copy.wait()
    gself_ref[...] = dot(grid_ref[...], wgs_ref[...]).astype(BF16)
    wm_copy.wait()
    off = off_ref[0]
    per = tile // LANES

    def step(t, carry):
        row = t * per
        lane0 = pl.multiple_of(t * tile, tile)
        send = columns([fs_ref[pl.ds(row + b, 1), :] - off for b in range(per)])
        recv = columns([sr_ref[pl.ds(row + b, 1), :] for b in range(per)])
        lhs = jnp.concatenate(
            [one_hot(send, ext), one_hot(recv, n), geo_columns(gsc[:, pl.ds(lane0, tile)])], axis=1
        )
        hidden = silu(dot(lhs, tab[...])).astype(BF16)
        msg[pl.ds(lane0, tile), :] = normalize(dot(hidden, wm_ref[...])).astype(BF16)
        return carry

    lax.fori_loop(0, edges // tile, step, 0)
    agg_ref[...] = dot(
        one_hot_t([sr_ref[b : b + 1, :] for b in range(edges // LANES)], n), msg[...]
    )
    far = lr_ref.shape[0]
    recv = columns([lr_ref[b : b + 1, :] for b in range(far)])
    lhs = jnp.concatenate([one_hot(recv, n), geo_columns(lsc[...])], axis=1)
    base_ref[...] = dot(lhs, tab[ext : ext + n + LANES, :]).astype(BF16)


def node_kernel(
    lr_ref, far_ref, agg_ref, base_ref, nself_ref, ws_ref, x_hbm, wm_hbm, wa_hbm, wo_hbm,
    out_ref, first_ref, last_ref, x_ref, wm_ref, wa_ref, wo_ref, sems,
):
    wm_copy, wa_copy, wo_copy, x_copy = fetch(
        [(wm_hbm, wm_ref), (wa_hbm, wa_ref), (wo_hbm, wo_ref), (x_hbm, x_ref)], sems
    )
    n = x_ref.shape[0]
    hidden = silu(dot(far_ref[...], ws_ref[...]) + base_ref[...].astype(F32)).astype(BF16)
    scatter = one_hot_t([lr_ref[b : b + 1, :] for b in range(lr_ref.shape[0])], n)
    wm_copy.wait()
    message = normalize(dot(hidden, wm_ref[...])).astype(BF16)
    aggregate = (agg_ref[...] + dot(scatter, message)).astype(BF16)
    wa_copy.wait()
    node_hidden = silu(nself_ref[...].astype(F32) + dot(aggregate, wa_ref[...])).astype(BF16)
    wo_copy.wait()
    x_copy.wait()
    fresh = (x_ref[...].astype(F32) + dot(node_hidden, wo_ref[...])).astype(BF16)
    out_ref[...] = fresh
    first_ref[...] = fresh[:BORDER]
    last_ref[...] = fresh[n - BORDER :]


def own_kernel(
    off_ref, ds_ref, geo_ref, wdgeo_ref, x_ref, wds_hbm, gproj_hbm, gself_hbm, wf_hbm, wga_hbm,
    fresh_hbm, pre_ref, gself_ref, wds_ref, wf_ref, wga_ref,
    tab, gsc, wsc, gproj_ref, sems,
):
    wds_copy, gproj_copy, gself_copy, wf_copy, wga_copy, fresh_copy = fetch(
        [
            (wds_hbm, wds_ref), (gproj_hbm, gproj_ref), (gself_hbm, gself_ref), (wf_hbm, wf_ref),
            (wga_hbm, wga_ref), (x_ref, fresh_hbm),
        ],
        sems,
    )
    n = x_ref.shape[0]
    vertices, points = ds_ref.shape
    features = geo_ref.shape[0] // vertices
    tab[n : n + LANES, :] = geo_table(wdgeo_ref, wsc)
    tab[n + LANES :, :] = jnp.zeros((LANES, tab.shape[1]), BF16)
    wds_copy.wait()
    tab[0:n, :] = dot(x_ref[...], wds_ref[...]).astype(BF16)
    gproj_copy.wait()
    start = off_ref[0] + BORDER
    for v in range(vertices):
        gsc[...] = jnp.zeros(gsc.shape, F32)
        for c in range(features):
            high, low = split(geo_ref[c * vertices + v : c * vertices + v + 1, :])
            gsc[c : c + 1, :] = high
            gsc[8 + c : 9 + c, :] = low
            gsc[16 + c : 17 + c, :] = high
        send = columns([ds_ref[v : v + 1, b : b + LANES] - start for b in range(0, points, LANES)])
        empty = jnp.zeros((points, LANES), BF16)
        lhs = jnp.concatenate([one_hot(send, n), geo_columns(gsc[...]), empty], axis=1)
        pre_ref[v * points : (v + 1) * points, :] = dot(lhs, tab[...]) + gproj_ref[...].astype(F32)
    gself_copy.wait()
    wf_copy.wait()
    wga_copy.wait()
    fresh_copy.wait()


def grid_kernel(
    off_ref, ds_ref, before_ref, after_ref, pre_ref, gself_ref, wds_ref, wf_ref, wga_ref, wp_ref,
    out_ref, *, nodes,
):
    vertices, points = ds_ref.shape
    halo = jnp.concatenate(
        [dot(before_ref[...], wds_ref[...]), dot(after_ref[...], wds_ref[...])], axis=0
    ).astype(BF16)
    off = off_ref[0]
    total = jnp.zeros((points, gself_ref.shape[1]), F32)
    for v in range(vertices):
        rows = []
        for b in range(0, points, LANES):
            place = ds_ref[v : v + 1, b : b + LANES] - off
            rows.append(
                jnp.where(place < BORDER, place, jnp.where(place >= BORDER + nodes, place - nodes, -1))
            )
        lhs = one_hot(columns(rows), 2 * BORDER)
        hidden = silu(dot(lhs, halo) + pre_ref[v * points : (v + 1) * points, :]).astype(BF16)
        total = total + normalize(dot(hidden, wf_ref[...]))
    hidden = silu(dot(total.astype(BF16), wga_ref[...]) + gself_ref[...].astype(F32)).astype(BF16)
    out_ref[...] = lax.dot_general(
        wp_ref[...], hidden, (((1,), (1,)), ((), ())), preferred_element_type=F32
    ).astype(BF16)


VM = pl.BlockSpec(memory_space=pltpu.MemorySpace.VMEM)
SM = pl.BlockSpec(memory_space=pltpu.MemorySpace.SMEM)
AN = pl.BlockSpec(memory_space=pltpu.MemorySpace.HBM)


def call(kernel, outs, ins, out_specs, scratch=(), mib=24, flops=0):
    return pl.pallas_call(
        kernel,
        out_shape=outs,
        in_specs=ins,
        out_specs=out_specs,
        scratch_shapes=list(scratch),
        compiler_params=pltpu.CompilerParams(vmem_limit_bytes=mib << 20),
        cost_estimate=pl.CostEstimate(flops=flops, transcendentals=0, bytes_accessed=1 << 22),
    )


def far_memory(*arrays):
    return [pltpu.with_memory_space_constraint(a, pltpu.MemorySpace.HBM) for a in arrays]


def swap(first, last):
    size = lax.axis_size("region")
    up = [(i, i + 1) for i in range(size - 1)]
    down = [(j, i) for i, j in up]
    return lax.ppermute(last, "region", up), lax.ppermute(first, "region", down)


def body(
    node_latent, grid_latent, fine_edge_sender, short_recv, short_geo, long_send, long_recv,
    long_geo, dec_send, dec_geo, w_send, w_recv, w_edge_geo, w_message, w_node_self, w_node_agg,
    w_node_out, w_dec_send, w_dec_grid, w_dec_geo, decoding_link_final_matrix, w_grid_agg,
    w_grid_self, final_projection_matrix,
):
    n, h = node_latent.shape
    points = grid_latent.shape[0]
    edges = fine_edge_sender.shape[0]
    far = long_send.shape[0]
    vertices = dec_send.shape[0]
    outputs = final_projection_matrix.shape[0]
    regions = lax.axis_size("region")
    slot = far // regions
    rings = regions // BLOCK
    offset = (lax.axis_index("region") * n - BORDER).astype(jnp.int32).reshape(1)

    classes = [[q + BLOCK * i for i in range(rings)] for q in range(BLOCK)]
    blocks = [[BLOCK * b + q for q in range(BLOCK)] for b in range(rings)]
    group = jnp.arange(regions, dtype=jnp.int32)
    wanted = jnp.maximum(long_send.reshape(regions, slot) - (group * n)[:, None], 0)
    wanted = (wanted + (group // BLOCK * COARSE)[:, None]).reshape(rings, BLOCK, slot)
    wanted = wanted.transpose(1, 0, 2).reshape(BLOCK, 1, rings * slot)
    wanted = jnp.broadcast_to(
        jnp.pad(wanted, ((0, 0), (0, 0), (0, LANES - rings * slot))), (BLOCK, 8, LANES)
    )
    asked = lax.all_to_all(
        wanted, "region", split_axis=0, concat_axis=0, tiled=True, axis_index_groups=blocks
    )
    before, after = swap(node_latent[:BORDER], node_latent[n - BORDER :])
    head, before, after = lax.optimization_barrier((node_latent[:COARSE], before, after))
    table = lax.all_gather(head, "region", axis=0, tiled=True, axis_index_groups=classes)
    whole = jax.ShapeDtypeStruct((n, h), BF16)
    weight = jax.ShapeDtypeStruct((h, h), BF16)
    rows = call(relay_kernel, jax.ShapeDtypeStruct((far, h), BF16), [VM, VM], VM, mib=8)(asked, table)
    rows, node_later = lax.optimization_barrier((rows, node_latent))
    fetched = lax.all_to_all(
        rows.reshape(BLOCK, far // BLOCK, h), "region",
        split_axis=0, concat_axis=0, tiled=True, axis_index_groups=blocks,
    ).reshape(far, h)

    target = jnp.where(long_send >= 0, long_recv, -1)
    target = target.reshape(rings, BLOCK, slot).transpose(1, 0, 2).reshape(far // LANES, LANES)
    far_geo = long_geo.reshape(-1, rings, BLOCK, slot).transpose(0, 2, 1, 3).reshape(-1, far)
    tile = 512
    ext = n + 2 * BORDER
    dense = pltpu.VMEM((h, h), BF16)
    field = jax.ShapeDtypeStruct((points, h), BF16)
    aggregate, base, node_self, send_weight, grid_proj, grid_self = call(
        functools.partial(fine_kernel, tile=tile),
        (jax.ShapeDtypeStruct((n, h), F32), jax.ShapeDtypeStruct((far, h), BF16), whole, weight, field, field),
        [SM] + [VM] * 8 + [AN] * 8,
        (VM,) * 6,
        [
            pltpu.VMEM((ext + n + LANES, h), BF16),
            pltpu.VMEM((edges, h), BF16),
            pltpu.VMEM((32, edges), F32),
            pltpu.VMEM((32, far), F32),
            pltpu.VMEM((32, h), F32),
            pltpu.VMEM((n, h), BF16),
            dense, dense, dense,
            pltpu.VMEM((points, h), BF16),
            dense, dense,
            pltpu.SemaphoreType.DMA((8,)),
        ],
        mib=28,
        flops=8 * edges * h * h,
    )(
        offset, fine_edge_sender.reshape(-1, LANES), short_recv.reshape(-1, LANES), short_geo,
        target, far_geo, before, after, w_edge_geo,
        *far_memory(
            node_later, w_send, w_recv, w_message, w_node_self, grid_latent, w_dec_grid, w_grid_self
        ),
    )
    border = jax.ShapeDtypeStruct((BORDER, h), BF16)
    fresh, first, last = call(
        node_kernel,
        (whole, border, border),
        [VM] * 6 + [AN] * 4,
        (VM,) * 3,
        [pltpu.VMEM((n, h), BF16), dense, dense, dense, pltpu.SemaphoreType.DMA((4,))],
        mib=16,
        flops=10 * n * h * h,
    )(
        target, fetched, aggregate, base, node_self, send_weight,
        *far_memory(node_later, w_message, w_node_agg, w_node_out),
    )
    before, after = swap(first, last)
    refreshed, pre, grid_self, dec_weight, final_weight, agg_weight = call(
        own_kernel,
        (
            whole, jax.ShapeDtypeStruct((vertices * points, h), F32),
            field, weight, weight, weight,
        ),
        [SM] + [VM] * 4 + [AN] * 5,
        (AN,) + (VM,) * 5,
        [
            pltpu.VMEM((n + 2 * LANES, h), BF16),
            pltpu.VMEM((32, points), F32),
            pltpu.VMEM((32, h), F32),
            pltpu.VMEM((points, h), BF16),
            pltpu.SemaphoreType.DMA((6,)),
        ],
        mib=20,
        flops=10 * n * h * h,
    )(
        offset, dec_send, dec_geo.reshape(-1, points), w_dec_geo, fresh,
        *far_memory(
            w_dec_send, grid_proj, grid_self, decoding_link_final_matrix, w_grid_agg
        ),
    )
    predicted = call(
        functools.partial(grid_kernel, nodes=n),
        jax.ShapeDtypeStruct((outputs, points), BF16),
        [SM] + [VM] * 9,
        VM,
        mib=20,
        flops=12 * n * h * h,
    )(
        offset, dec_send, before, after, pre, grid_self, dec_weight, final_weight, agg_weight,
        final_projection_matrix,
    )
    return (refreshed, predicted)


def solution(mesh):
    rows = P(("ens", "region"), None)
    line = P(("ens", "region"))
    in_specs = (
        rows, rows, line, line, P(None, ("ens", "region")), line, line, P(None, ("ens", "region")),
        P(None, ("ens", "region")), P(None, None, ("ens", "region")),
    ) + (P(),) * 14
    out_specs = (rows, P(None, ("ens", "region")))
    return jax.shard_map(body, mesh=mesh, in_specs=in_specs, out_specs=out_specs, check_vma=False)
```

```python
import functools

import jax
import jax.numpy as jnp
from jax import lax
from jax.experimental import pallas as pl
from jax.experimental.pallas import tpu as pltpu
from jax.sharding import PartitionSpec as P

BORDER = 64
COARSE = 64
BLOCK = 8
LANES = 128
F32 = jnp.float32
BF16 = jnp.bfloat16


def dot(left, right):
    return jnp.dot(left, right, preferred_element_type=F32)


def silu(v):
    half = 0.5 * v
    return half + half * jnp.tanh(half)


def normalize(values):
    inv = 1.0 / values.shape[-1]
    centred = values - jnp.sum(values, axis=-1, keepdims=True) * inv
    spread = jnp.sum(centred * centred, axis=-1, keepdims=True) * inv
    return centred * lax.rsqrt(spread + 1e-05)


def columns(rows):
    return jnp.concatenate(
        [jnp.broadcast_to(r, (LANES, LANES)).T for r in rows], axis=0
    )


def one_hot(cols, width):
    lane = lax.broadcasted_iota(jnp.int32, cols.shape, 1)
    return jnp.concatenate(
        [jnp.where(cols == lane + k, 1.0, 0.0).astype(BF16) for k in range(0, width, LANES)], axis=1
    )


def one_hot_t(rows, height):
    node = lax.broadcasted_iota(jnp.int32, (height, LANES), 0)
    return jnp.concatenate([jnp.where(node == r, 1.0, 0.0).astype(BF16) for r in rows], axis=1)


def split(values):
    high = values.astype(BF16).astype(F32)
    return high, values - high


def geo_columns(stack):
    n = stack.shape[1]
    full = jnp.concatenate([stack, jnp.zeros((LANES - 32, n), F32)], axis=0)
    return jnp.concatenate(
        [full[:, b : b + LANES].T for b in range(0, n, LANES)], axis=0
    ).astype(BF16)


def fill_geo(ref, first, second, third):
    ref[...] = jnp.zeros(ref.shape, F32)
    n = first.shape[0]
    ref[0:n, :] = first
    ref[8 : 8 + n, :] = second
    ref[16 : 16 + n, :] = third


def geo_table(wref, scratch):
    high, low = split(wref[...])
    fill_geo(scratch, high, high, low)
    rows = scratch[...]
    return jnp.concatenate([rows, jnp.zeros((LANES - 32, rows.shape[1]), F32)], axis=0).astype(BF16)


def fetch(pairs, sems):
    copies = [pltpu.make_async_copy(src, dst, sems.at[i]) for i, (src, dst) in enumerate(pairs)]
    for copy in copies:
        copy.start()
    return copies


def relay_kernel(asked_ref, table_ref, out_ref):
    rows = out_ref.shape[0] // asked_ref.shape[0]
    cols = jnp.concatenate(
        [columns([asked_ref[q, 0:1, :]])[:rows] for q in range(asked_ref.shape[0])], axis=0
    )
    out_ref[...] = dot(one_hot(cols, table_ref.shape[0]), table_ref[...]).astype(BF16)


def fine_kernel(
    off_ref, fs_ref, sr_ref, geo_ref, lr_ref, lgeo_ref, before_ref, after_ref, weg_ref,
    x_hbm, ws_hbm, wr_hbm, wm_hbm, wself_hbm, grid_hbm, wdg_hbm, wgs_hbm,
    agg_ref, base_ref, nself_ref, ws_ref, gproj_hbm, gself_hbm,
    tab, msg, gsc, lsc, wsc, x_ref, wr_ref, wm_ref, wself_ref, grid_ref, wdg_ref, wgs_ref,
    gproj_ref, gself_ref, sems, out_sems, *, tile,
):
    x_copy, ws_copy, wr_copy, wm_copy, wself_copy, grid_copy, wdg_copy, wgs_copy = fetch(
        [
            (x_hbm, x_ref), (ws_hbm, ws_ref), (wr_hbm, wr_ref), (wm_hbm, wm_ref),
            (wself_hbm, wself_ref), (grid_hbm, grid_ref), (wdg_hbm, wdg_ref), (wgs_hbm, wgs_ref),
        ],
        sems,
    )
    n, h = x_ref.shape
    edges = geo_ref.shape[1]
    ext = n + 2 * BORDER
    tab[ext + n : ext + n + LANES, :] = geo_table(weg_ref, wsc)
    high, low = split(geo_ref[...])
    fill_geo(gsc, high, low, high)
    high, low = split(lgeo_ref[...])
    fill_geo(lsc, high, low, high)
    x_copy.wait()
    ws_copy.wait()
    x = x_ref[...]
    tab[0:BORDER, :] = dot(before_ref[...], ws_ref[...]).astype(BF16)
    tab[BORDER : BORDER + n, :] = dot(x, ws_ref[...]).astype(BF16)
    tab[BORDER + n : ext, :] = dot(after_ref[...], ws_ref[...]).astype(BF16)
    wr_copy.wait()
    tab[ext : ext + n, :] = dot(x, wr_ref[...]).astype(BF16)
    wself_copy.wait()
    nself_ref[...] = dot(x, wself_ref[...]).astype(BF16)
    grid_copy.wait()
    wdg_copy.wait()
    gproj_ref[...] = dot(grid_ref[...], wdg_ref[...]).astype(BF16)
    wgs_copy.wait()
    gself_ref[...] = dot(grid_ref[...], wgs_ref[...]).astype(BF16)
    stores = fetch([(gproj_ref, gproj_hbm), (gself_ref, gself_hbm)], out_sems)
    wm_copy.wait()
    off = off_ref[0]
    per = tile // LANES

    def step(t, carry):
        row = t * per
        lane0 = pl.multiple_of(t * tile, tile)
        send = columns([fs_ref[pl.ds(row + b, 1), :] - off for b in range(per)])
        recv = columns([sr_ref[pl.ds(row + b, 1), :] for b in range(per)])
        lhs = jnp.concatenate(
            [one_hot(send, ext), one_hot(recv, n), geo_columns(gsc[:, pl.ds(lane0, tile)])], axis=1
        )
        hidden = silu(dot(lhs, tab[...])).astype(BF16)
        msg[pl.ds(lane0, tile), :] = normalize(dot(hidden, wm_ref[...])).astype(BF16)
        return carry

    lax.fori_loop(0, edges // tile, step, 0)
    agg_ref[...] = dot(
        one_hot_t([sr_ref[b : b + 1, :] for b in range(edges // LANES)], n), msg[...]
    )
    far = lr_ref.shape[0]
    recv = columns([lr_ref[b : b + 1, :] for b in range(far)])
    lhs = jnp.concatenate([one_hot(recv, n), geo_columns(lsc[...])], axis=1)
    base_ref[...] = dot(lhs, tab[ext : ext + n + LANES, :]).astype(BF16)
    for store in stores:
        store.wait()


def node_kernel(
    lr_ref, far_ref, agg_ref, base_ref, nself_ref, ws_ref, x_hbm, wm_hbm, wa_hbm, wo_hbm,
    out_ref, first_ref, last_ref, x_ref, wm_ref, wa_ref, wo_ref, sems,
):
    wm_copy, wa_copy, wo_copy, x_copy = fetch(
        [(wm_hbm, wm_ref), (wa_hbm, wa_ref), (wo_hbm, wo_ref), (x_hbm, x_ref)], sems
    )
    n = x_ref.shape[0]
    hidden = silu(dot(far_ref[...], ws_ref[...]) + base_ref[...].astype(F32)).astype(BF16)
    scatter = one_hot_t([lr_ref[b : b + 1, :] for b in range(lr_ref.shape[0])], n)
    wm_copy.wait()
    message = normalize(dot(hidden, wm_ref[...])).astype(BF16)
    aggregate = (agg_ref[...] + dot(scatter, message)).astype(BF16)
    wa_copy.wait()
    node_hidden = silu(nself_ref[...].astype(F32) + dot(aggregate, wa_ref[...])).astype(BF16)
    wo_copy.wait()
    x_copy.wait()
    fresh = (x_ref[...].astype(F32) + dot(node_hidden, wo_ref[...])).astype(BF16)
    out_ref[...] = fresh
    first_ref[...] = fresh[:BORDER]
    last_ref[...] = fresh[n - BORDER :]


def own_kernel(
    off_ref, ds_ref, geo_ref, wdgeo_ref, x_ref, wds_hbm, gproj_hbm, gself_hbm, wf_hbm, wga_hbm,
    fresh_hbm, pre_ref, gself_ref, wds_ref, wf_ref, wga_ref,
    tab, gsc, wsc, gproj_ref, sems,
):
    wds_copy, gproj_copy, gself_copy, wf_copy, wga_copy, fresh_copy = fetch(
        [
            (wds_hbm, wds_ref), (gproj_hbm, gproj_ref), (gself_hbm, gself_ref), (wf_hbm, wf_ref),
            (wga_hbm, wga_ref), (x_ref, fresh_hbm),
        ],
        sems,
    )
    n = x_ref.shape[0]
    vertices, points = ds_ref.shape
    features = geo_ref.shape[0] // vertices
    tab[n : n + LANES, :] = geo_table(wdgeo_ref, wsc)
    tab[n + LANES :, :] = jnp.zeros((LANES, tab.shape[1]), BF16)
    wds_copy.wait()
    tab[0:n, :] = dot(x_ref[...], wds_ref[...]).astype(BF16)
    gproj_copy.wait()
    start = off_ref[0] + BORDER
    for v in range(vertices):
        gsc[...] = jnp.zeros(gsc.shape, F32)
        for c in range(features):
            high, low = split(geo_ref[c * vertices + v : c * vertices + v + 1, :])
            gsc[c : c + 1, :] = high
            gsc[8 + c : 9 + c, :] = low
            gsc[16 + c : 17 + c, :] = high
        send = columns([ds_ref[v : v + 1, b : b + LANES] - start for b in range(0, points, LANES)])
        empty = jnp.zeros((points, LANES), BF16)
        lhs = jnp.concatenate([one_hot(send, n), geo_columns(gsc[...]), empty], axis=1)
        pre_ref[v * points : (v + 1) * points, :] = dot(lhs, tab[...]) + gproj_ref[...].astype(F32)
    gself_copy.wait()
    wf_copy.wait()
    wga_copy.wait()
    fresh_copy.wait()


def grid_kernel(
    off_ref, ds_ref, before_ref, after_ref, pre_ref, gself_ref, wds_ref, wf_ref, wga_ref, wp_ref,
    out_ref, *, nodes,
):
    vertices, points = ds_ref.shape
    halo = jnp.concatenate(
        [dot(before_ref[...], wds_ref[...]), dot(after_ref[...], wds_ref[...])], axis=0
    ).astype(BF16)
    off = off_ref[0]
    total = jnp.zeros((points, gself_ref.shape[1]), F32)
    for v in range(vertices):
        rows = []
        for b in range(0, points, LANES):
            place = ds_ref[v : v + 1, b : b + LANES] - off
            rows.append(
                jnp.where(place < BORDER, place, jnp.where(place >= BORDER + nodes, place - nodes, -1))
            )
        lhs = one_hot(columns(rows), 2 * BORDER)
        hidden = silu(dot(lhs, halo) + pre_ref[v * points : (v + 1) * points, :]).astype(BF16)
        total = total + normalize(dot(hidden, wf_ref[...]))
    hidden = silu(dot(total.astype(BF16), wga_ref[...]) + gself_ref[...].astype(F32)).astype(BF16)
    out_ref[...] = lax.dot_general(
        wp_ref[...], hidden, (((1,), (1,)), ((), ())), preferred_element_type=F32
    ).astype(BF16)


VM = pl.BlockSpec(memory_space=pltpu.MemorySpace.VMEM)
SM = pl.BlockSpec(memory_space=pltpu.MemorySpace.SMEM)
AN = pl.BlockSpec(memory_space=pltpu.MemorySpace.HBM)


def call(kernel, outs, ins, out_specs, scratch=(), mib=24, flops=0):
    return pl.pallas_call(
        kernel,
        out_shape=outs,
        in_specs=ins,
        out_specs=out_specs,
        scratch_shapes=list(scratch),
        compiler_params=pltpu.CompilerParams(vmem_limit_bytes=mib << 20),
        cost_estimate=pl.CostEstimate(flops=flops, transcendentals=0, bytes_accessed=1 << 22),
    )


def far_memory(*arrays):
    return [pltpu.with_memory_space_constraint(a, pltpu.MemorySpace.HBM) for a in arrays]


def swap(first, last):
    size = lax.axis_size("region")
    up = [(i, i + 1) for i in range(size - 1)]
    down = [(j, i) for i, j in up]
    return lax.ppermute(last, "region", up), lax.ppermute(first, "region", down)


def body(
    node_latent, grid_latent, fine_edge_sender, short_recv, short_geo, long_send, long_recv,
    long_geo, dec_send, dec_geo, w_send, w_recv, w_edge_geo, w_message, w_node_self, w_node_agg,
    w_node_out, w_dec_send, w_dec_grid, w_dec_geo, decoding_link_final_matrix, w_grid_agg,
    w_grid_self, final_projection_matrix,
):
    n, h = node_latent.shape
    points = grid_latent.shape[0]
    edges = fine_edge_sender.shape[0]
    far = long_send.shape[0]
    vertices = dec_send.shape[0]
    outputs = final_projection_matrix.shape[0]
    regions = lax.axis_size("region")
    slot = far // regions
    rings = regions // BLOCK
    offset = (lax.axis_index("region") * n - BORDER).astype(jnp.int32).reshape(1)

    classes = [[q + BLOCK * i for i in range(rings)] for q in range(BLOCK)]
    blocks = [[BLOCK * b + q for q in range(BLOCK)] for b in range(rings)]
    group = jnp.arange(regions, dtype=jnp.int32)
    wanted = jnp.maximum(long_send.reshape(regions, slot) - (group * n)[:, None], 0)
    wanted = (wanted + (group // BLOCK * COARSE)[:, None]).reshape(rings, BLOCK, slot)
    wanted = wanted.transpose(1, 0, 2).reshape(BLOCK, 1, rings * slot)
    wanted = jnp.broadcast_to(
        jnp.pad(wanted, ((0, 0), (0, 0), (0, LANES - rings * slot))), (BLOCK, 8, LANES)
    )
    asked = lax.all_to_all(
        wanted, "region", split_axis=0, concat_axis=0, tiled=True, axis_index_groups=blocks
    )
    before, after = swap(node_latent[:BORDER], node_latent[n - BORDER :])
    head, before, after = lax.optimization_barrier((node_latent[:COARSE], before, after))
    table = lax.all_gather(head, "region", axis=0, tiled=True, axis_index_groups=classes)
    whole = jax.ShapeDtypeStruct((n, h), BF16)
    weight = jax.ShapeDtypeStruct((h, h), BF16)
    rows = call(relay_kernel, jax.ShapeDtypeStruct((far, h), BF16), [VM, VM], VM, mib=8)(asked, table)
    rows, node_later = lax.optimization_barrier((rows, node_latent))
    fetched = lax.all_to_all(
        rows.reshape(BLOCK, far // BLOCK, h), "region",
        split_axis=0, concat_axis=0, tiled=True, axis_index_groups=blocks,
    ).reshape(far, h)

    target = jnp.where(long_send >= 0, long_recv, -1)
    target = target.reshape(rings, BLOCK, slot).transpose(1, 0, 2).reshape(far // LANES, LANES)
    far_geo = long_geo.reshape(-1, rings, BLOCK, slot).transpose(0, 2, 1, 3).reshape(-1, far)
    tile = 1024
    ext = n + 2 * BORDER
    dense = pltpu.VMEM((h, h), BF16)
    field = pltpu.MemorySpace.HBM((points, h), BF16)
    aggregate, base, node_self, send_weight, grid_proj, grid_self = call(
        functools.partial(fine_kernel, tile=tile),
        (jax.ShapeDtypeStruct((n, h), F32), jax.ShapeDtypeStruct((far, h), BF16), whole, weight, field, field),
        [SM] + [VM] * 8 + [AN] * 8,
        (VM,) * 4 + (AN,) * 2,
        [
            pltpu.VMEM((ext + n + LANES, h), BF16),
            pltpu.VMEM((edges, h), BF16),
            pltpu.VMEM((32, edges), F32),
            pltpu.VMEM((32, far), F32),
            pltpu.VMEM((32, h), F32),
            pltpu.VMEM((n, h), BF16),
            dense, dense, dense,
            pltpu.VMEM((points, h), BF16),
            dense, dense,
            pltpu.VMEM((points, h), BF16),
            pltpu.VMEM((points, h), BF16),
            pltpu.SemaphoreType.DMA((8,)),
            pltpu.SemaphoreType.DMA((2,)),
        ],
        mib=28,
        flops=8 * edges * h * h,
    )(
        offset, fine_edge_sender.reshape(-1, LANES), short_recv.reshape(-1, LANES), short_geo,
        target, far_geo, before, after, w_edge_geo,
        *far_memory(
            node_later, w_send, w_recv, w_message, w_node_self, grid_latent, w_dec_grid, w_grid_self
        ),
    )
    border = jax.ShapeDtypeStruct((BORDER, h), BF16)
    fresh, first, last = call(
        node_kernel,
        (whole, border, border),
        [VM] * 6 + [AN] * 4,
        (VM,) * 3,
        [pltpu.VMEM((n, h), BF16), dense, dense, dense, pltpu.SemaphoreType.DMA((4,))],
        mib=16,
        flops=10 * n * h * h,
    )(
        target, fetched, aggregate, base, node_self, send_weight,
        *far_memory(node_later, w_message, w_node_agg, w_node_out),
    )
    before, after = swap(first, last)
    refreshed, pre, grid_self, dec_weight, final_weight, agg_weight = call(
        own_kernel,
        (
            whole, jax.ShapeDtypeStruct((vertices * points, h), F32),
            jax.ShapeDtypeStruct((points, h), BF16), weight, weight, weight,
        ),
        [SM] + [VM] * 4 + [AN] * 5,
        (AN,) + (VM,) * 5,
        [
            pltpu.VMEM((n + 2 * LANES, h), BF16),
            pltpu.VMEM((32, points), F32),
            pltpu.VMEM((32, h), F32),
            pltpu.VMEM((points, h), BF16),
            pltpu.SemaphoreType.DMA((6,)),
        ],
        mib=20,
        flops=10 * n * h * h,
    )(
        offset, dec_send, dec_geo.reshape(-1, points), w_dec_geo, fresh,
        *far_memory(
            w_dec_send, grid_proj, grid_self, decoding_link_final_matrix, w_grid_agg
        ),
    )
    predicted = call(
        functools.partial(grid_kernel, nodes=n),
        jax.ShapeDtypeStruct((outputs, points), BF16),
        [SM] + [VM] * 9,
        VM,
        mib=20,
        flops=12 * n * h * h,
    )(
        offset, dec_send, before, after, pre, grid_self, dec_weight, final_weight, agg_weight,
        final_projection_matrix,
    )
    return (refreshed, predicted)


def solution(mesh):
    rows = P(("ens", "region"), None)
    line = P(("ens", "region"))
    in_specs = (
        rows, rows, line, line, P(None, ("ens", "region")), line, line, P(None, ("ens", "region")),
        P(None, ("ens", "region")), P(None, None, ("ens", "region")),
    ) + (P(),) * 14
    out_specs = (rows, P(None, ("ens", "region")))
    return jax.shard_map(body, mesh=mesh, in_specs=in_specs, out_specs=out_specs, check_vma=False)
```
